256 devices in a mesh: dp: 8 (over z_lo, core), vocab: 32 (over z_hi, x, y).
Axes of the slice: x: 4, y: 4, z: 8 (z_hi: 2, z_lo: 4; z = z_hi * 4 + z_lo), core: 2. Of those that a mesh axis runs over, the one named last changes fastest.
Arguments:
- policy_hidden: bfloat16 [1024, 4096], P('dp'), may hold values from -84 to 84
- policy_weight: bfloat16 [4096, 65536], P('dp', 'vocab'), may hold values from -0.09375 to 0.09375
- reference_hidden: bfloat16 [1024, 4096], P(('dp', 'vocab')), may hold values from -84 to 84
- reference_weight: bfloat16 [4096, 65536], P(None, ('dp', 'vocab')), may hold values from -0.09375 to 0.09375
- targets: int32 [1024], replicated, may hold values from 0 to 65535
- response_mask: int32 [1024], replicated, may hold values 0 or 1
- pair_index: int32 [32], replicated, may hold values from 0 to 31, each once
Outputs:
- hidden_grad: bfloat16 [1024, 4096], P('vocab', 'dp')
- weight_grad: bfloat16 [4096, 65536], P('dp', 'vocab')
- total_loss: float32 [], replicated
The draws below stay inside these ranges and needn't reach their ends.
Inputs may be any that keep to these rules, and one draw needn't show every extreme that they name: `pair_index`: each number of 0 to 31 once; entries 2p and 2p + 1 are the chosen and the rejected sequence of pair p.
All inputs are finite; a program needn't handle non-finite values.
Results may differ from the reference program's by a relative error of at most 0.005.
The reference program's roundings to bfloat16 on the way (of `logit_grad`) count: a program that leaves them out, or rounds other values in their place, can miss the bound.
Values may be sent and summed in bfloat16 or wider, within the bound.
A program may use at most 128 MiB of HBM per device.

```python
import math
import jax
import jax.numpy as jnp
import numpy as np
from jax import lax

D = 4096
VOCAB = 65536
SEQ_LEN = 32
SEQS = 32
TOKENS = 1024


def scaled_rows(key, salt):
    folded = jax.random.fold_in(key, salt)
    key_value = jax.random.fold_in(folded, 1)
    return 3.0 * jnp.clip(jax.random.normal(key_value, (TOKENS, D), jnp.float32), -6.0, 6.0)


def draw_policy_hidden(key, part):
    return scaled_rows(key, 11).astype(jnp.bfloat16)


def draw_reference_hidden(key, part):
    return scaled_rows(key, 23).astype(jnp.bfloat16)


def touch_ends(array, stream_key, smallest, top_value):
    longest = array.shape.index(max(array.shape))
    spots = []
    for shift in (0, 1):
        where = [jax.random.randint(jax.random.fold_in(stream_key, axis), (), 0, length) for axis, length in enumerate(array.shape)]
        where[longest] = (where[longest] + shift) % array.shape[longest]
        spots.append(tuple(where))
    return array.at[spots[0]].set(smallest).at[spots[1]].set(top_value)


def levels(stream_key, shape, cuts, least, high):
    def one(axis_at, parts):
        steps = jax.random.uniform(jax.random.fold_in(jax.random.fold_in(stream_key, 6), axis_at), (parts,), jnp.float32, least / len(cuts), high / len(cuts))
        return jnp.repeat(jnp.exp(steps), shape[axis_at] // parts).reshape((-1,) + (1,) * (len(shape) - axis_at - 1))

    level = one(*cuts[0])
    for cut in cuts[1:]:
        level = level * one(*cut)
    return level


def rank_bounds(amount, skew):
    weights = [(1 << 20) // math.isqrt(standing ** skew) + 1 for standing in range(1, amount + 1)]
    scale = 1 + sum(weights) // (1 << 30)
    return np.cumsum(np.array([max(1, weight // scale) for weight in weights]))


def skewed_ids(stream_key, dims, amount, slope):
    listing = rank_bounds(amount, slope)
    lot = jax.random.randint(jax.random.fold_in(stream_key, 1), dims, 0, int(listing[amount - 1]))
    standing = jnp.searchsorted(jnp.asarray(listing, jnp.int32), lot, side="right")
    return jax.random.permutation(jax.random.fold_in(stream_key, 2), amount)[standing].astype(jnp.int32)


def scatter_about(key, dims, scale, reach, shards=(), kind=jnp.bfloat16):
    array = jax.random.normal(key, dims, jnp.float32) * scale
    if len(shards) > 0:
        array = levels(key, dims, shards, -0.22, 0.18) * array
    return jnp.clip(array, min=-reach, max=reach).astype(kind)


def setup_inputs(seed: int = 0) -> dict:
    key_of = jax.random.split(jax.random.key(seed), 8)
    policy_hidden = draw_policy_hidden(jax.random.fold_in(key_of[7], 71), 0)
    policy_weight = scatter_about(key_of[1], (D, VOCAB), D ** -0.5, 0.09375, ((0, 8), (1, 32)))
    reference_hidden = draw_reference_hidden(jax.random.fold_in(key_of[7], 71), 0)
    reference_weight = scatter_about(key_of[3], (D, VOCAB), D ** -0.5, 0.09375, ((1, 256),))
    targets = touch_ends(skewed_ids(key_of[4], (TOKENS,), VOCAB, 2), jax.random.fold_in(key_of[4], 3), 0, VOCAB - 1).astype(jnp.int32)
    response_mask = touch_ends((jax.random.randint(key_of[5], (TOKENS,), 0, 4) < 3).astype(jnp.int32), jax.random.fold_in(key_of[5], 1), 0, 1)
    pair_index = jax.random.permutation(key_of[6], SEQS).astype(jnp.int32)
    return {"policy_hidden": policy_hidden, "policy_weight": policy_weight, "reference_hidden": reference_hidden, "reference_weight": reference_weight, "targets": targets, "response_mask": response_mask, "pair_index": pair_index}


beta = 0.1
loss_scale = 4096.0
block_size = 64


def pair_terms(log_ratio, pair_index):
    chosen = pair_index[0::2]
    rejected = pair_index[1::2]
    margin = beta * (log_ratio[chosen] - log_ratio[rejected])
    pair_count = chosen.shape[0]
    total_loss = jnp.sum(jax.nn.softplus(-margin)) / pair_count
    weight = -beta * loss_scale * jax.nn.sigmoid(-margin) / pair_count
    numbers = jnp.arange(log_ratio.shape[0], dtype=jnp.int32)[:, None]
    factor = jnp.sum(jnp.where(numbers == chosen[None, :], weight[None, :], 0.0) - jnp.where(numbers == rejected[None, :], weight[None, :], 0.0), axis=1)
    return total_loss, factor


def token_logp(hidden, weight, targets):
    blocks = hidden.shape[0] // block_size

    def block_logp(inputs):
        row_block, target_block = inputs
        logits = jnp.dot(row_block, weight, preferred_element_type=jnp.float32)
        largest = jnp.max(logits, axis=1)
        exp_total = jnp.sum(jnp.exp(logits - largest[:, None]), axis=1)
        picked = jnp.take_along_axis(logits, target_block[:, None], axis=1)[:, 0]
        return picked - largest - jnp.log(exp_total)

    return lax.map(block_logp, (hidden.reshape(blocks, block_size, hidden.shape[1]), targets.reshape(blocks, block_size))).reshape(-1)


def reference(policy_hidden, policy_weight, reference_hidden, reference_weight, targets, response_mask, pair_index):
    policy_logp = token_logp(policy_hidden, policy_weight, targets)
    reference_logp = token_logp(reference_hidden, reference_weight, targets)
    active = response_mask.astype(jnp.float32)
    log_ratio = jnp.sum((active * (policy_logp - reference_logp)).reshape(-1, SEQ_LEN), axis=1)
    total_loss, factor = pair_terms(log_ratio, pair_index)
    token_scale = active * jnp.repeat(factor, SEQ_LEN)
    blocks = policy_hidden.shape[0] // block_size
    vocab_ids = lax.broadcasted_iota(jnp.int32, (block_size, policy_weight.shape[1]), 1)

    def backward(weight_grad, inputs):
        row_block, target_block, scale_block = inputs
        logits = jnp.dot(row_block, policy_weight, preferred_element_type=jnp.float32)
        largest = jnp.max(logits, axis=1, keepdims=True)
        log_total = largest + jnp.log(jnp.sum(jnp.exp(logits - largest), axis=1, keepdims=True))
        onehot = (vocab_ids == target_block[:, None]).astype(jnp.float32)
        logit_grad = (scale_block[:, None] * (onehot - jnp.exp(logits - log_total))).astype(jnp.bfloat16)
        weight_grad = weight_grad + jnp.dot(row_block.T, logit_grad, preferred_element_type=jnp.float32)
        row_grad = jnp.dot(logit_grad, policy_weight.T, preferred_element_type=jnp.float32).astype(jnp.bfloat16)
        return weight_grad, row_grad

    weight_grad, hidden_grad = lax.scan(backward, jnp.zeros(policy_weight.shape, jnp.float32), (policy_hidden.reshape(blocks, block_size, policy_hidden.shape[1]), targets.reshape(blocks, block_size), token_scale.reshape(blocks, block_size)))
    return hidden_grad.reshape(policy_hidden.shape), weight_grad.astype(jnp.bfloat16), total_loss
```

```python
import jax
import jax.numpy as jnp
from jax import lax
from jax.sharding import Mesh
from jax.sharding import PartitionSpec as P

SEQ_LEN = 32
DP = ("dp_0", "dp_1")
VOCAB = ("vocab_0", "vocab_1", "vocab_2")
DP_VOCAB = ("dp_0", "dp_1", "vocab_0", "vocab_1", "vocab_2")


beta = 0.1
loss_scale = 4096.0


def all_in_one(value, axis):
    leaves = jax.tree.leaves(value)
    order = sorted(range(len(leaves)), key=lambda k: -leaves[k].size)
    width = (1, *leaves[order[0]].shape)[-1]
    lines = [
        jnp.pad(leaves[k].reshape(-1), (0, -leaves[k].size % width)).reshape(-1, width)
        for k in order
    ]
    both, at, found = (lax.all_gather(jnp.concatenate(lines), axis), 0, {})
    for k, line in zip(order, lines):
        slab = both[:, at : at + len(line)].reshape(len(both), -1)
        found[k] = slab[:, : leaves[k].size].reshape(-1, *leaves[k].shape)
        at += len(line)
    numbers = iter(range(len(leaves)))
    return jax.tree.map(lambda _: found[next(numbers)], value)


def merged_by_axis(value, axes, combine):
    for axis in axes:
        pieces = all_in_one(value, axis)
        value = jax.tree.map(lambda part: part[0], pieces)
        for k in range(1, lax.axis_size(axis)):
            value = combine(value, jax.tree.map(lambda part: part[k], pieces))
    return value


def in_blocks(value, dim, peers):
    shape = value.shape
    tiles = value.reshape(*shape[:dim], peers, shape[dim] // peers, *shape[dim + 1 :])
    return jnp.moveaxis(tiles, dim, 0)


def sum_at_owner(value, axis, dim):
    peers = lax.axis_size(axis)
    tiles = lax.all_to_all(in_blocks(value, dim, peers), axis, 0, 0, tiled=True)
    return jnp.sum(tiles, axis=0)


def pair_terms(log_ratio, pair_index):
    chosen = pair_index[0::2]
    rejected = pair_index[1::2]
    margin = beta * (log_ratio[chosen] - log_ratio[rejected])
    pair_count = chosen.shape[0]
    total_loss = jnp.sum(jax.nn.softplus(-margin)) / pair_count
    weight = -beta * loss_scale * jax.nn.sigmoid(-margin) / pair_count
    numbers = jnp.arange(log_ratio.shape[0], dtype=jnp.int32)[:, None]
    factor = jnp.sum(
        jnp.where(numbers == chosen[None, :], weight[None, :], 0.0)
        - jnp.where(numbers == rejected[None, :], weight[None, :], 0.0),
        axis=1,
    )
    return (total_loss, factor)


def local_pick(logits, targets, offset, axis):
    column_ids = lax.broadcasted_iota(jnp.int32, logits.shape, axis)
    shifted = targets - offset
    wanted = shifted[:, None] if axis == 1 else shifted[None, :]
    return jnp.sum(jnp.where(column_ids == wanted, logits, 0.0), axis=axis)


def merge_pair(earlier, later):
    largest = jnp.maximum(earlier[0], later[0])
    exp_total = earlier[1] * jnp.exp(earlier[0] - largest) + later[1] * jnp.exp(later[0] - largest)
    return (largest, exp_total, earlier[2] + later[2])


def merge_heads(earlier, later):
    return merge_pair(earlier[0:3], later[0:3]) + merge_pair(earlier[3:6], later[3:6])


def local(
    policy_hidden,
    policy_weight,
    reference_hidden,
    reference_weight,
    targets,
    response_mask,
    pair_index,
):
    data_index = lax.axis_index(DP)
    vocab_index = lax.axis_index(VOCAB)
    vocab_devices = lax.axis_size(VOCAB)
    data_devices = lax.axis_size(DP)
    policy_width = policy_weight.shape[1]
    reference_width = reference_weight.shape[1]
    active = response_mask.astype(jnp.float32)
    columns = lax.all_to_all(policy_hidden, DP, split_axis=1, concat_axis=0, tiled=True)
    reference_rows = reference_hidden
    for axis in ("dp_0", "vocab_0", "vocab_2", "vocab_1", "dp_1"):
        reference_rows = lax.all_gather(reference_rows, axis, axis=0, tiled=True)
    reference_logits = jnp.dot(
        reference_rows,
        reference_weight,
        preferred_element_type=jnp.float32,
    )
    reference_targets = targets.reshape(4, 2, 2, 4, 4, 4).transpose(1, 3, 4, 2, 0, 5).reshape(-1)

    def in_order(value):
        return value.reshape(2, 4, 4, 2, 4, 4).transpose(4, 0, 3, 1, 2, 5).reshape(-1)

    reference_offset = (data_index * vocab_devices + vocab_index) * reference_width
    reference_top = jnp.max(reference_logits, axis=1)
    reference_pick = local_pick(reference_logits, reference_targets, reference_offset, 1)
    slice_width = policy_width // data_devices
    weight_block = policy_weight
    policy_logits = lax.psum_scatter(
        lax.dot_general(
            weight_block, columns, (((0,), (1,)), ((), ())), preferred_element_type=jnp.float32
        ),
        DP,
        scatter_dimension=0,
        tiled=True,
    )
    policy_offset = vocab_index * policy_width + data_index * slice_width
    policy_top = jnp.max(policy_logits, axis=0)
    policy_pick = local_pick(policy_logits, targets, policy_offset, 0)
    local_stats = (
        policy_top,
        jnp.sum(jnp.exp(policy_logits - policy_top[None, :]), axis=0),
        policy_pick,
        in_order(reference_top),
        in_order(jnp.sum(jnp.exp(reference_logits - reference_top[:, None]), axis=1)),
        in_order(reference_pick),
    )
    merged = merged_by_axis(local_stats, DP_VOCAB, merge_heads)
    policy_total = merged[0] + jnp.log(merged[1])
    reference_logp = merged[5] - merged[3] - jnp.log(merged[4])
    log_ratio = jnp.sum(
        (active * (merged[2] - policy_total - reference_logp)).reshape(-1, SEQ_LEN), axis=1
    )
    total_loss, factor = pair_terms(log_ratio, pair_index)
    token_scale = active * jnp.repeat(factor, SEQ_LEN)
    row_ids = lax.broadcasted_iota(jnp.int32, policy_logits.shape, 0)
    onehot = (row_ids == (targets - policy_offset)[None, :]).astype(jnp.float32)
    logit_grad = (
        token_scale[None, :] * (onehot - jnp.exp(policy_logits - policy_total[None, :]))
    ).astype(jnp.bfloat16)
    segment = lax.all_gather(logit_grad, DP, axis=0, tiled=True)
    weight_block = policy_weight
    column_grad = lax.dot_general(
        columns, segment, (((0,), (1,)), ((), ())), preferred_element_type=jnp.float32
    )
    hidden_part = lax.dot_general(
        segment, weight_block, (((0,), (1,)), ((), ())), preferred_element_type=jnp.float32
    )
    weight_grad, hidden_part = (column_grad, hidden_part)
    hidden_grad = sum_at_owner(hidden_part, VOCAB, 0)
    return (hidden_grad.astype(jnp.bfloat16), weight_grad.astype(jnp.bfloat16), total_loss)


def solution(mesh):
    torus = Mesh(
        mesh.devices.reshape(4, 2, 2, 4, 4), ("dp_0", "dp_1", "vocab_0", "vocab_1", "vocab_2")
    )
    in_specs = (P(DP, None), P(DP, VOCAB), P(DP_VOCAB, None), P(None, DP_VOCAB), P(), P(), P())
    out_specs = (P(VOCAB, DP), P(DP, VOCAB), P())
    return jax.shard_map(local, mesh=torus, in_specs=in_specs, out_specs=out_specs, check_vma=False)
```
